256 devices in a mesh: rows: 128 (over z, y, x_lo, core), grp: 2 (over x_hi).
Axes of the slice: x: 4 (x_hi: 2, x_lo: 2; x = x_hi * 2 + x_lo), y: 4, z: 8, core: 2. Of those that a mesh axis runs over, the one named last changes fastest.
Arguments:
- region_id: int32 [1048576], P(('rows', 'grp')), may hold values from 0 to 63
- product_id: int32 [1048576], P(('rows', 'grp')), may hold values from 0 to 63
- measures: bfloat16 [1048576, 256], P(('rows', 'grp')), may hold values from -1 to 1
- slot_of_cell: int32 [4096], replicated, may hold values from 0 to 4095, each once
Outputs:
- cube: float32 [4096, 256], P(('rows', 'grp'))
- region_totals: float32 [64, 256], replicated
- product_totals: float32 [64, 256], replicated
The draws below stay inside these ranges and needn't reach their ends.
All inputs are finite; a program needn't handle non-finite values.
Results may differ from the reference program's by a relative error of at most 0.0003.
Values sent between devices are 32-bit elements; how exact they have to be, the bound alone decides.
No kernel may reach another device: no remote copies, remote signals or barrier semaphores. Data moves between devices by JAX's collectives and lax.ppermute only.
A program may use at most 64 MiB of HBM per device.

```python
import math
import jax
import jax.numpy as jnp
import numpy as np

REGIONS = 64
PRODUCTS = 64
MEASURE_COUNT = 256
CELLS = 4096
FACT_ROW_TOTAL = 1048576


def draw_measures(key, part):
    position = jnp.arange(FACT_ROW_TOTAL, dtype=jnp.float32) / max(FACT_ROW_TOTAL - 1, 1)
    spread_amount = (0.05 * (1.0 + 2.0 * position))[:, None]
    measure_values = jax.random.normal(key, (FACT_ROW_TOTAL, MEASURE_COUNT), jnp.float32) * spread_amount
    return jnp.clip(measure_values, -1.0, 1.0).astype(jnp.bfloat16)


def touch_ends(entries, own_key, smallest, high):
    shape = entries.shape
    spot = [jax.random.randint(jax.random.fold_in(own_key, axis), (), 0, shape[axis]) for axis in range(len(shape))]
    entries = entries.at[tuple(spot)].set(smallest)
    longest = shape.index(max(shape))
    spot[longest] = (spot[longest] + 1) % shape[longest]
    return entries.at[tuple(spot)].set(high)


def rank_bounds(amount, skew):
    portions = [(1 << 20) // math.isqrt(rank ** skew) + 1 for rank in range(1, amount + 1)]
    scale = 1 + sum(portions) // (1 << 30)
    return np.cumsum(np.array([max(1, weight // scale) for weight in portions]))


def skewed_ids(stream_key, dims, number_of, lean):
    listing = rank_bounds(number_of, lean)
    lot = jax.random.randint(jax.random.fold_in(stream_key, 1), dims, 0, int(listing[number_of - 1]))
    grade = jnp.searchsorted(jnp.asarray(listing, jnp.int32), lot, side="right")
    return jax.random.permutation(jax.random.fold_in(stream_key, 2), number_of)[grade].astype(jnp.int32)


def setup_inputs(seed: int = 0) -> dict:
    arg_keys = jax.random.split(jax.random.key(seed), 5)
    region_id = touch_ends(skewed_ids(arg_keys[0], (FACT_ROW_TOTAL,), REGIONS, 2), jax.random.fold_in(arg_keys[0], 3), 0, REGIONS - 1).astype(jnp.int32)
    product_id = touch_ends(skewed_ids(arg_keys[1], (FACT_ROW_TOTAL,), PRODUCTS, 1), jax.random.fold_in(arg_keys[1], 3), 0, PRODUCTS - 1).astype(jnp.int32)
    measures = draw_measures(jax.random.fold_in(arg_keys[4], 71), 0)
    slot_of_cell = jax.random.permutation(arg_keys[3], CELLS).astype(jnp.int32)
    return {"region_id": region_id, "product_id": product_id, "measures": measures, "slot_of_cell": slot_of_cell}


def reference(region_id, product_id, measures, slot_of_cell):
    values = measures.astype(jnp.float32)
    cell = region_id * PRODUCTS + product_id
    slot = jnp.take(slot_of_cell, cell)
    cube = jax.ops.segment_sum(values, slot, num_segments=CELLS)
    region_totals = jax.ops.segment_sum(values, region_id, num_segments=REGIONS)
    product_totals = jax.ops.segment_sum(values, product_id, num_segments=PRODUCTS)
    return cube, region_totals, product_totals
```

```python
import functools

import jax
import jax.numpy as jnp
from jax import lax
from jax.experimental import pallas as pl
from jax.experimental.pallas import tpu as pltpu
from jax.sharding import Mesh
from jax.sharding import PartitionSpec as P

Z, Y, XL, CORE, XH = "rows_0", "rows_1", "rows_2", "rows_3", "grp"
ALL = (Z, Y, XL, CORE, XH)
PLANE = (Y, XL, XH)
PLANE_CORES = (Y, XL, CORE, XH)
WIDTH = 256
SIDE = 64
BF16, F32 = jnp.bfloat16, jnp.float32
VMEM = pl.BlockSpec(memory_space=pltpu.VMEM)
SMEM = pl.BlockSpec(memory_space=pltpu.SMEM)


def prep_body(core_ref, region_ref, product_ref, table_ref, group_ref, line_ref):
    table = table_ref[...]
    high, low = table >> 6, table & 63
    line = (high >> 3) * 8 + (low & 7)
    plane = (high & 7) * 2 + ((low >> 4) & 1)
    group = ((low >> 3) & 1) * 32 + ((low >> 5) ^ core_ref[0]) * 16 + plane
    both = jnp.concatenate([group, line], axis=1).astype(F32).astype(BF16)
    label = lax.broadcasted_iota(jnp.int32, (SIDE, region_ref.shape[1]), 0)
    in_region = (label == region_ref[...]).astype(F32).astype(BF16)
    found = lax.dot_general(both, in_region, (((0,), (0,)), ((), ())), preferred_element_type=F32)
    in_product = label == product_ref[...]
    for half, out in ((found[:SIDE], group_ref), (found[SIDE:], line_ref)):
        out[...] = jnp.sum(jnp.where(in_product, half, 0.0), axis=0, keepdims=True).astype(jnp.int32)


def prep(core, region, product, table):
    row = jax.ShapeDtypeStruct(region.shape, jnp.int32)
    return pl.pallas_call(
        prep_body,
        out_shape=[row, row],
        in_specs=[SMEM, VMEM, VMEM, VMEM],
        out_specs=[VMEM, VMEM],
        cost_estimate=pl.CostEstimate(flops=2 * 10**9, bytes_accessed=10**5, transcendentals=0),
        name="prep",
    )(core, region, product, table)


def block_body(first, per_dot, with_totals, adds, *refs):
    refs = list(refs)
    group_ref, line_ref, measures_ref = refs[:3]
    del refs[:3]
    label_ref = refs.pop(0) if with_totals else None
    other_ref = refs.pop(0) if adds else None
    out_ref, one_line, lhs = refs
    n = group_ref.shape[1]
    label = lax.broadcasted_iota(jnp.int32, (SIDE, n), 0)
    one_line[...] = (label == line_ref[...]).astype(F32).astype(BF16)

    def step(b, _):
        for k in range(per_dot):
            chosen = (group_ref[...] == first + b * per_dot + k).astype(F32).astype(BF16)
            lhs[k * SIDE : (k + 1) * SIDE, :] = one_line[...] * chosen
        sums = jnp.dot(lhs[...], measures_ref[...], preferred_element_type=F32)
        for k in range(per_dot):
            piece = sums[k * SIDE : (k + 1) * SIDE]
            if adds:
                piece = piece + other_ref[b * per_dot + k, 0:SIDE, :]
            out_ref[b * per_dot + k, 0:SIDE, :] = piece
        return 0

    lax.fori_loop(0, 16 // per_dot, step, 0)
    if with_totals:
        member = (label == label_ref[...]).astype(F32).astype(BF16)
        totals = jnp.dot(member, measures_ref[...], preferred_element_type=F32)
        for g in range(16):
            piece = totals[4 * g : 4 * g + 4]
            if adds:
                piece = piece + other_ref[g, SIDE : SIDE + 4, :]
            out_ref[g, SIDE : SIDE + 4, :] = piece
            out_ref[g, SIDE + 4 : SIDE + 8, :] = jnp.zeros((4, WIDTH), F32)


def block(first, group, line, measures, label=None, other=None):
    per_dot = 8
    n = group.shape[1]
    height = SIDE if label is None else SIDE + 8
    args = [group, line, measures] + [a for a in (label, other) if a is not None]
    return pl.pallas_call(
        functools.partial(block_body, first, per_dot, label is not None, other is not None),
        out_shape=jax.ShapeDtypeStruct((16, height, WIDTH), F32),
        in_specs=[VMEM] * len(args),
        out_specs=VMEM,
        scratch_shapes=[pltpu.VMEM((SIDE, n), BF16), pltpu.VMEM((SIDE * per_dot, n), BF16)],
        compiler_params=pltpu.CompilerParams(vmem_limit_bytes=24 << 20),
        cost_estimate=pl.CostEstimate(
            flops=2 * 1024 * n * WIDTH, bytes_accessed=3 << 20, transcendentals=0
        ),
        name="block",
    )(*args)


def to_partner(array):
    return lax.ppermute(array, CORE, [(0, 1), (1, 0)])


def exchange(array, axes):
    return lax.all_to_all(array, axes, 0, 0, tiled=True)


def on_device(region_id, product_id, measures, slot_of_cell):
    core = lax.axis_index(CORE)
    region, product = region_id[None, :], product_id[None, :]
    group, line = prep(core[None], region, product, slot_of_cell.reshape(SIDE, SIDE))
    kept_label = jnp.where(core == 0, region, product)
    sent_label = jnp.where(core == 0, product, region)
    after = lax.optimization_barrier

    sent_a = block(16, group, line, measures, label=sent_label)
    got_a = to_partner(sent_a)
    group, sent_a = after((group, sent_a))
    sent_b = block(48, group, line, measures)
    got_b = to_partner(sent_b)
    group, sent_b, got_a = after((group, sent_b, got_a))
    chip_a = block(0, group, line, measures, label=kept_label, other=got_a)
    near_a = exchange(chip_a, PLANE)
    group, chip_a, got_b = after((group, chip_a, got_b))
    chip_b = block(32, group, line, measures, other=got_b)
    near_b = exchange(chip_b, PLANE)

    column_a = jnp.sum(near_a, axis=0)
    totals = jnp.broadcast_to(column_a[SIDE:][None], (8, 8, WIDTH))
    far_a = exchange(jnp.concatenate([column_a[:SIDE].reshape(8, 8, WIDTH), totals], axis=1), Z)
    column_b = jnp.sum(near_b, axis=0)
    far_b = exchange(column_b.reshape(8, 8, WIDTH), Z)
    cube_a = jnp.sum(far_a, axis=0)
    spread = exchange(jnp.broadcast_to(cube_a[None, 8:12], (32, 4, WIDTH)), PLANE_CORES)
    cube = jnp.concatenate([cube_a[:8], jnp.sum(far_b, axis=0)], axis=0)
    spread = spread.reshape(8, 2, 2, 4, WIDTH).swapaxes(0, 1).reshape(2, SIDE, WIDTH)
    return cube, spread[0], spread[1]


def solution(mesh):
    split = Mesh(mesh.devices.reshape(8, 4, 2, 2, mesh.shape["grp"]), ALL)
    in_specs = (P(ALL), P(ALL), P(ALL, None), P())
    out_specs = (P(ALL, None), P(), P())
    return jax.shard_map(
        on_device, mesh=split, in_specs=in_specs, out_specs=out_specs, check_vma=False
    )
```

```python
import functools

import jax
import jax.numpy as jnp
from jax import lax
from jax.experimental import pallas as pl
from jax.experimental.pallas import tpu as pltpu
from jax.sharding import Mesh
from jax.sharding import PartitionSpec as P


Z, Y, XL, CORE, XH = "rows_0", "rows_1", "rows_2", "rows_3", "grp"
ALL = (Z, Y, XL, CORE, XH)
PLANE = (Y, XL, XH)
WIDTH = 256
SIDE = 64
PEERS = 16
LAYERS = 8
OWN = 16
PIECE = LAYERS * OWN
TOTALS = 2 * SIDE // LAYERS
HALF = PEERS // 2
BF16, F32 = jnp.bfloat16, jnp.float32
VMEM = pl.BlockSpec(memory_space=pltpu.VMEM)
SMEM = pl.BlockSpec(memory_space=pltpu.SMEM)
PARAMS = pltpu.CompilerParams(vmem_limit_bytes=24 << 20)


def cost(rows, n):
    return pl.CostEstimate(flops=2 * rows * n * WIDTH, bytes_accessed=1 << 20, transcendentals=0)


def sum_body(cell_ref, measures_ref, totals_ref):
    cell = cell_ref[...]
    label = lax.broadcasted_iota(jnp.int32, (SIDE, cell.shape[1]), 0)
    in_region = (label == (cell >> 6)).astype(F32).astype(BF16)
    in_product = (label == (cell & 63)).astype(F32).astype(BF16)
    member = jnp.concatenate([in_region, in_product], axis=0)
    totals = jnp.dot(member, measures_ref[...], preferred_element_type=F32)
    totals_ref[...] = totals.reshape(LAYERS, TOTALS, WIDTH)


def sum_labels(cell, measures):
    return pl.pallas_call(
        sum_body,
        out_shape=jax.ShapeDtypeStruct((LAYERS, TOTALS, WIDTH), F32),
        in_specs=[VMEM, VMEM],
        out_specs=VMEM,
        compiler_params=PARAMS,
        cost_estimate=cost(128, cell.shape[1]),
        name="sum_labels",
    )(cell, measures)


def prep_body(core_ref, cell_ref, table_ref, code_ref):
    slot = table_ref[...]
    far = ((slot >> 5) & 1) ^ core_ref[0]
    plane = ((slot >> 6) & 7) * 2 + ((slot >> 4) & 1)
    high = far * 32 + plane * 2 + (slot >> 11)
    low = ((slot >> 9) & 3) * 16 + (slot & 15)
    both = jnp.concatenate([high * 64, low], axis=0).astype(F32).astype(BF16)
    cell = cell_ref[...]
    label = lax.broadcasted_iota(jnp.int32, (SIDE, cell.shape[1]), 0)
    in_line = ((label & 31) == (cell >> 7)).astype(F32).astype(BF16)
    found = lax.dot_general(both, in_line, (((0,), (0,)), ((), ())), preferred_element_type=F32)
    place = lax.broadcasted_iota(jnp.int32, found.shape, 0) == (cell & 127)
    code_ref[...] = jnp.sum(jnp.where(place, found, 0.0), axis=0, keepdims=True).astype(jnp.int32)


def prep(core, cell, table):
    return pl.pallas_call(
        prep_body,
        out_shape=jax.ShapeDtypeStruct(cell.shape, jnp.int32),
        in_specs=[SMEM, VMEM, VMEM],
        out_specs=VMEM,
        compiler_params=PARAMS,
        cost_estimate=cost(256, cell.shape[1]),
        name="prep",
    )(core, cell, table)


def half_sums(first, code_ref, measures_ref, line_ref, lhs_ref):
    group = code_ref[...] >> 6
    for k in range(2 * HALF):
        chosen = (group == first + k).astype(F32).astype(BF16)
        lhs_ref[k * SIDE : (k + 1) * SIDE, :] = line_ref[...] * chosen
    return jnp.dot(lhs_ref[...], measures_ref[...], preferred_element_type=F32)


def set_lines(code_ref, line_ref):
    label = lax.broadcasted_iota(jnp.int32, line_ref.shape, 0)
    line_ref[...] = (label == (code_ref[...] & 63)).astype(F32).astype(BF16)


def send_body(first, code_ref, measures_ref, out_ref, line_ref, lhs_ref):
    set_lines(code_ref, line_ref)
    sums = half_sums(first, code_ref, measures_ref, line_ref, lhs_ref)
    out_ref[...] = sums.reshape(HALF, PIECE, WIDTH)


def scratch(n):
    return [pltpu.VMEM((SIDE, n), BF16), pltpu.VMEM((HALF * PIECE, n), BF16)]


def send(first, code, measures):
    n = code.shape[1]
    return pl.pallas_call(
        functools.partial(send_body, first),
        out_shape=jax.ShapeDtypeStruct((HALF, PIECE, WIDTH), F32),
        in_specs=[VMEM, VMEM],
        out_specs=VMEM,
        scratch_shapes=scratch(n),
        compiler_params=PARAMS,
        cost_estimate=cost(HALF * PIECE, n),
        name="send",
    )(code, measures)


def keep_body(code_ref, measures_ref, got0_ref, got1_ref, totals_ref, out_ref, line_ref, lhs_ref):
    set_lines(code_ref, line_ref)
    for half, got_ref in enumerate((got0_ref, got1_ref)):
        sums = half_sums(half * 2 * HALF, code_ref, measures_ref, line_ref, lhs_ref)
        out_ref[half * HALF : (half + 1) * HALF, 0:PIECE, :] = (
            sums.reshape(HALF, PIECE, WIDTH) + got_ref[...]
        )
    totals = jnp.sum(totals_ref[...], axis=0)
    for peer in range(PEERS):
        out_ref[peer, PIECE:, :] = totals


def keep(code, measures, got0, got1, totals):
    n = code.shape[1]
    return pl.pallas_call(
        keep_body,
        out_shape=jax.ShapeDtypeStruct((PEERS, PIECE + TOTALS, WIDTH), F32),
        in_specs=[VMEM] * 5,
        out_specs=VMEM,
        scratch_shapes=scratch(n),
        compiler_params=PARAMS,
        cost_estimate=cost(PEERS * PIECE, n),
        name="keep",
    )(code, measures, got0, got1, totals)


def column_body(near_ref, out_ref):
    out_ref[:, 0:OWN, :] = jnp.sum(near_ref[:, 0:PIECE, :], axis=0).reshape(LAYERS, OWN, WIDTH)
    totals = jnp.sum(near_ref[:, PIECE:, :], axis=0)
    for layer in range(LAYERS):
        out_ref[layer, OWN:, :] = totals


def column(near):
    return pl.pallas_call(
        column_body,
        out_shape=jax.ShapeDtypeStruct((LAYERS, OWN + TOTALS, WIDTH), F32),
        in_specs=[VMEM],
        out_specs=VMEM,
        compiler_params=PARAMS,
        name="column",
    )(near)


def last_body(far_ref, cube_ref, totals_ref):
    totals_ref[...] = far_ref[:, OWN:, :].reshape(2 * SIDE, WIDTH)
    cube_ref[...] = jnp.sum(far_ref[:, 0:OWN, :], axis=0)


def last(far):
    return pl.pallas_call(
        last_body,
        out_shape=[
            jax.ShapeDtypeStruct((OWN, WIDTH), F32),
            jax.ShapeDtypeStruct((2 * SIDE, WIDTH), F32),
        ],
        in_specs=[VMEM],
        out_specs=[VMEM, VMEM],
        compiler_params=PARAMS,
        name="last",
    )(far)


def both_body(mine_ref, other_ref, region_ref, product_ref):
    region_ref[...] = mine_ref[0:SIDE, :] + other_ref[0:SIDE, :]
    product_ref[...] = mine_ref[SIDE:, :] + other_ref[SIDE:, :]


def both(mine, other):
    total = jax.ShapeDtypeStruct((SIDE, WIDTH), F32)
    return pl.pallas_call(
        both_body,
        out_shape=[total, total],
        in_specs=[VMEM, VMEM],
        out_specs=[VMEM, VMEM],
        compiler_params=PARAMS,
        name="both",
    )(mine, other)


def to_partner(array):
    return lax.ppermute(array, CORE, [(0, 1), (1, 0)])


def exchange(array, axes):
    return lax.all_to_all(array, axes, 0, 0, tiled=True)


def on_device(region_id, product_id, measures, slot_of_cell):
    core = lax.axis_index(CORE)
    table = slot_of_cell.reshape(32, 128)
    cell = (region_id * SIDE + product_id)[None, :]
    totals = sum_labels(cell, measures)
    layer_totals = exchange(totals, Z)
    code = prep(core[None], cell, table)
    sent0 = send(32, code, measures)
    got0 = to_partner(sent0)
    code, sent0 = lax.optimization_barrier((code, sent0))
    sent1 = send(48, code, measures)
    got1 = to_partner(sent1)
    chip = keep(code, measures, got0, got1, layer_totals)
    far = exchange(column(exchange(chip, PLANE)), Z)
    cube, mine = last(far)
    region_totals, product_totals = both(mine, to_partner(mine))
    return cube, region_totals, product_totals


def solution(mesh):
    split = Mesh(mesh.devices.reshape(8, 4, 2, 2, mesh.shape["grp"]), ALL)
    in_specs = (P(ALL), P(ALL), P(ALL, None), P())
    out_specs = (P(ALL, None), P(), P())
    return jax.shard_map(
        on_device, mesh=split, in_specs=in_specs, out_specs=out_specs, check_vma=False
    )
```

```python
import functools

import jax
import jax.numpy as jnp
from jax import lax
from jax.experimental import pallas as pl
from jax.experimental.pallas import tpu as pltpu
from jax.sharding import Mesh
from jax.sharding import PartitionSpec as P


ALL = "all"
WIDTH = 256
SIDE = 64
OWN = 16
PEERS = 8
LATER = 16
PIECE = LATER * OWN
TOTALS = 2 * SIDE // LATER
HALF = PEERS // 2
PER_DOT = HALF * PIECE // SIDE
BF16, F32 = jnp.bfloat16, jnp.float32
VMEM = pl.BlockSpec(memory_space=pltpu.VMEM)
SMEM = pl.BlockSpec(memory_space=pltpu.SMEM)
PARAMS = pltpu.CompilerParams(vmem_limit_bytes=20 << 20)


def device(z, y, x, core):
    return (((z % 8 * 4 + y) * 2 + x % 2) * 2 + core) * 2 + x // 2


def member(core, a, pair, b, rest):
    return device(rest * 2 + pair + core, *((b, a) if core else (a, b)), core)


CHOICES = [(core, i, j) for core in range(2) for i in range(4) for j in range(4)]
FIRST = [
    [member(core, a, pair, b, rest) for a in range(4) for pair in range(2)]
    for core, b, rest in CHOICES
]
SECOND = [
    [member(core, a, pair, b, rest) for b in range(4) for rest in range(4)]
    for core, a, pair in [(c, i, j) for c in range(2) for i in range(4) for j in range(2)]
]
PARTNERS = [(d, d ^ 2) for d in range(256)]


def cost(rows, n):
    return pl.CostEstimate(flops=2 * rows * n * WIDTH, bytes_accessed=1 << 20, transcendentals=0)


def sum_body(cell_ref, measures_ref, totals_ref):
    cell = cell_ref[...]
    label = lax.broadcasted_iota(jnp.int32, (SIDE, cell.shape[1]), 0)
    in_region = (label == (cell >> 6)).astype(F32).astype(BF16)
    in_product = (label == (cell & 63)).astype(F32).astype(BF16)
    member = jnp.concatenate([in_region, in_product], axis=0)
    totals = jnp.dot(member, measures_ref[...], preferred_element_type=F32)
    totals_ref[...] = totals.reshape(LATER, TOTALS, WIDTH)


def sum_labels(cell, measures):
    return pl.pallas_call(
        sum_body,
        out_shape=jax.ShapeDtypeStruct((LATER, TOTALS, WIDTH), F32),
        in_specs=[VMEM, VMEM],
        out_specs=VMEM,
        compiler_params=PARAMS,
        cost_estimate=cost(128, cell.shape[1]),
        name="sum_labels",
    )(cell, measures)


def prep_body(core_ref, cell_ref, table_ref, code_ref):
    slot = table_ref[...]
    core = (slot >> 5) & 1
    y = (slot >> 7) & 3
    x = ((slot >> 4) & 1) * 2 + ((slot >> 6) & 1)
    z = ((slot >> 9) - core) & 7
    a, b = jnp.where(core == 0, y, x), jnp.where(core == 0, x, y)
    high = (core ^ core_ref[0]) * 32 + a * 8 + (z & 1) * 4 + b
    low = (z >> 1) * 16 + (slot & 15)
    both = jnp.concatenate([high * 64, low], axis=0).astype(F32).astype(BF16)
    cell = cell_ref[...]
    label = lax.broadcasted_iota(jnp.int32, (SIDE, cell.shape[1]), 0)
    in_line = ((label & 31) == (cell >> 7)).astype(F32).astype(BF16)
    found = lax.dot_general(both, in_line, (((0,), (0,)), ((), ())), preferred_element_type=F32)
    place = lax.broadcasted_iota(jnp.int32, found.shape, 0) == (cell & 127)
    code_ref[...] = jnp.sum(jnp.where(place, found, 0.0), axis=0, keepdims=True).astype(jnp.int32)


def prep(core, cell, table):
    return pl.pallas_call(
        prep_body,
        out_shape=jax.ShapeDtypeStruct(cell.shape, jnp.int32),
        in_specs=[SMEM, VMEM, VMEM],
        out_specs=VMEM,
        compiler_params=PARAMS,
        cost_estimate=cost(256, cell.shape[1]),
        name="prep",
    )(core, cell, table)


def half_sums(first, code_ref, measures_ref, line_ref, lhs_ref):
    group = code_ref[...] >> 6
    for k in range(PER_DOT):
        chosen = (group == first + k).astype(F32).astype(BF16)
        lhs_ref[k * SIDE : (k + 1) * SIDE, :] = line_ref[...] * chosen
    return jnp.dot(lhs_ref[...], measures_ref[...], preferred_element_type=F32)


def set_lines(code_ref, line_ref):
    label = lax.broadcasted_iota(jnp.int32, line_ref.shape, 0)
    line_ref[...] = (label == (code_ref[...] & 63)).astype(F32).astype(BF16)


def block_body(first, code_ref, measures_ref, out_ref, line_ref, lhs_ref):
    set_lines(code_ref, line_ref)
    for half in range(2):
        sums = half_sums(first + half * PER_DOT, code_ref, measures_ref, line_ref, lhs_ref)
        out_ref[half * HALF : (half + 1) * HALF] = sums.reshape(HALF, PIECE, WIDTH)


def block(first, code, measures):
    n = code.shape[1]
    return pl.pallas_call(
        functools.partial(block_body, first),
        out_shape=jax.ShapeDtypeStruct((PEERS, PIECE, WIDTH), F32),
        in_specs=[VMEM, VMEM],
        out_specs=VMEM,
        scratch_shapes=[pltpu.VMEM((SIDE, n), BF16), pltpu.VMEM((HALF * PIECE, n), BF16)],
        compiler_params=PARAMS,
        cost_estimate=cost(PEERS * PIECE, n),
        name="block",
    )(code, measures)


def join_body(mine_ref, got_ref, totals_ref, out_ref):
    out_ref[:, 0:PIECE, :] = mine_ref[...] + got_ref[...]
    totals = jnp.sum(totals_ref[...], axis=0)
    for peer in range(PEERS):
        out_ref[peer, PIECE:, :] = totals


def join(mine, got, totals):
    return pl.pallas_call(
        join_body,
        out_shape=jax.ShapeDtypeStruct((PEERS, PIECE + TOTALS, WIDTH), F32),
        in_specs=[VMEM] * 3,
        out_specs=VMEM,
        compiler_params=PARAMS,
        name="join",
    )(mine, got, totals)


def column_body(near_ref, out_ref):
    out_ref[:, 0:OWN, :] = jnp.sum(near_ref[:, 0:PIECE, :], axis=0).reshape(LATER, OWN, WIDTH)
    totals = jnp.sum(near_ref[:, PIECE:, :], axis=0)
    for layer in range(LATER):
        out_ref[layer, OWN:, :] = totals


def column(near):
    return pl.pallas_call(
        column_body,
        out_shape=jax.ShapeDtypeStruct((LATER, OWN + TOTALS, WIDTH), F32),
        in_specs=[VMEM],
        out_specs=VMEM,
        compiler_params=PARAMS,
        name="column",
    )(near)


def last_body(far_ref, cube_ref, totals_ref):
    totals_ref[...] = far_ref[:, OWN:, :].reshape(2 * SIDE, WIDTH)
    cube_ref[...] = jnp.sum(far_ref[:, 0:OWN, :], axis=0)


def last(far):
    return pl.pallas_call(
        last_body,
        out_shape=[
            jax.ShapeDtypeStruct((OWN, WIDTH), F32),
            jax.ShapeDtypeStruct((2 * SIDE, WIDTH), F32),
        ],
        in_specs=[VMEM],
        out_specs=[VMEM, VMEM],
        compiler_params=PARAMS,
        name="last",
    )(far)


def both_body(mine_ref, other_ref, region_ref, product_ref):
    region_ref[...] = mine_ref[0:SIDE, :] + other_ref[0:SIDE, :]
    product_ref[...] = mine_ref[SIDE:, :] + other_ref[SIDE:, :]


def both(mine, other):
    total = jax.ShapeDtypeStruct((SIDE, WIDTH), F32)
    return pl.pallas_call(
        both_body,
        out_shape=[total, total],
        in_specs=[VMEM, VMEM],
        out_specs=[VMEM, VMEM],
        compiler_params=PARAMS,
        name="both",
    )(mine, other)


def to_partner(array):
    return lax.ppermute(array, ALL, PARTNERS)


def exchange(array, groups):
    return lax.all_to_all(array, ALL, 0, 0, axis_index_groups=groups, tiled=True)


def on_device(region_id, product_id, measures, slot_of_cell):
    core = (lax.axis_index(ALL) >> 1) & 1
    table = slot_of_cell.reshape(32, 128)
    cell = (region_id * SIDE + product_id)[None, :]
    totals = sum_labels(cell, measures)
    some_totals = exchange(totals, SECOND)
    code = prep(core[None], cell, table)
    sent = block(32, code, measures)
    got = to_partner(sent)
    code, sent, some_totals = lax.optimization_barrier((code, sent, some_totals))
    mine = block(0, code, measures)
    chip = join(mine, got, some_totals)
    far = exchange(column(exchange(chip, FIRST)), SECOND)
    cube, mine = last(far)
    region_totals, product_totals = both(mine, to_partner(mine))
    return cube, region_totals, product_totals


def solution(mesh):
    split = Mesh(mesh.devices.reshape(-1), (ALL,))
    in_specs = (P(ALL), P(ALL), P(ALL, None), P(None))
    out_specs = (P(ALL, None), P(), P())
    return jax.shard_map(
        on_device, mesh=split, in_specs=in_specs, out_specs=out_specs, check_vma=False
    )
```
